768 devices in a mesh: section: 32 (over y, z_lo), fsdp: 24 (over x, z_hi, core).
Axes of the slice: x: 4, y: 8, z: 12 (z_hi: 3, z_lo: 4; z = z_hi * 4 + z_lo), core: 2. Of those that a mesh axis runs over, the one named last changes fastest.
Arguments:
- source_rows: bfloat16 [12288, 4096], P(('section', 'fsdp')), may hold values from -6 to 6
- target_rows: bfloat16 [4096, 4096], P('section'), may hold values from -6 to 6
- attn_weights: bfloat16 [32, 4, 4096, 3072], P('section', None, None, 'fsdp'), may hold values from -3.76875 to 3.76875
- gains: float32 [32, 4096], P('section'), may hold values from 0.25 to 1.75
- lengths: int32 [32], P('section'), may hold values from 192 to 384
Outputs:
- source_next: bfloat16 [12288, 4096], P(('section', 'fsdp'))
- target_next: bfloat16 [4096, 4096], P('section')
The draws below stay inside these ranges and needn't reach their ends.
Inputs may be any that keep to these rules, and one draw needn't show every extreme that they name: Keys at positions lengths[s] and beyond are padding.
All inputs are finite; a program needn't handle non-finite values.
Results may differ from the reference program's by a relative error of at most 0.015.
The reference program's roundings to bfloat16 on the way count: a program that leaves them out, or rounds other values in their place, can miss the bound.
Values may be sent and summed in bfloat16 or wider, within the bound.
A program may use at most 64 MiB of HBM per device.

```python
import math
import jax
import jax.numpy as jnp
from jax import lax

D = 4096
HEAD_DIM = 64
IN_LEN = 384
OUT_LEN = 128
INNER = 3072
SOURCE_TOTAL = 12288
TARGET_TOTAL = 4096
N_SECTION = 32
N_FSDP = 24


def draw_attn_weights(key, part):
    shape_all = (N_SECTION, 4, D, INNER)
    drawn = jnp.clip(jax.random.normal(key, shape_all, jnp.float32), -6.0, 6.0) / math.sqrt(D)
    return drawn.astype(jnp.bfloat16)


def touch_ends(array, stream_key, least, high):
    longest = array.shape.index(max(array.shape))
    spots = []
    for shift in (0, 1):
        where = [jax.random.randint(jax.random.fold_in(stream_key, axis), (), 0, length) for axis, length in enumerate(array.shape)]
        where[longest] = (where[longest] + shift) % array.shape[longest]
        spots.append(tuple(where))
    return array.at[spots[0]].set(least).at[spots[1]].set(high)


def block_levels(rng, extent, shards, smallest, high):
    gain, own = 1.0, jax.random.fold_in(rng, 6)
    for position, parts in shards:
        draws = jnp.exp(jax.random.uniform(jax.random.fold_in(own, position), (parts,), jnp.float32, smallest / len(shards), high / len(shards)))
        gain = gain * jnp.repeat(draws, extent[position] // parts).reshape([-1 if axis == position else 1 for axis in range(len(extent))])
    return gain


def centred(stream_key, shape, deviation, limit, split=(), kind=jnp.bfloat16):
    result = deviation * jax.random.normal(stream_key, shape, jnp.float32)
    if split:
        result = result * block_levels(stream_key, shape, split, -0.22, 0.18)
    return jnp.clip(result, -limit, limit).astype(kind)


def setup_inputs(seed: int = 0) -> dict:
    keys = jax.random.split(jax.random.key(seed), 6)
    source_rows = centred(keys[0], (SOURCE_TOTAL, D), 1.0, 6.0, ((0, 768),))
    target_rows = centred(keys[1], (TARGET_TOTAL, D), 1.0, 6.0, ((0, 32),))
    attn_weights = draw_attn_weights(jax.random.fold_in(keys[5], 71), 0)
    gains = jnp.clip(1.0 + 0.15 * jax.random.normal(keys[3], (N_SECTION, D), jnp.float32), 0.25, 1.75)
    lengths = touch_ends(jax.random.randint(keys[4], (N_SECTION,), IN_LEN // 2, IN_LEN + 1), jax.random.fold_in(keys[4], 1), IN_LEN // 2, IN_LEN).astype(jnp.int32)
    return dict(source_rows=source_rows, target_rows=target_rows, attn_weights=attn_weights, gains=gains, lengths=lengths)


def rms_norm(block_rows, gain_row):
    widened = block_rows.astype(jnp.float32)
    inverse_rms = lax.rsqrt(lax.optimization_barrier(jnp.mean(widened * widened, axis=-1, keepdims=True)) + 1e-06)
    return (widened * inverse_rms * gain_row).astype(jnp.bfloat16)

def project(block_rows, weight):
    return jnp.dot(block_rows, weight, preferred_element_type=jnp.float32).astype(jnp.bfloat16)

def attend(queries, key_rows, values, length):
    query_count = queries.shape[0]
    key_count = key_rows.shape[0]
    head_count = queries.shape[1] // HEAD_DIM
    query_heads = queries.reshape(query_count, head_count, HEAD_DIM).astype(jnp.float32)
    key_heads = key_rows.reshape(key_count, head_count, HEAD_DIM).astype(jnp.float32)
    value_heads = values.reshape(key_count, head_count, HEAD_DIM).astype(jnp.float32)
    scores = jnp.einsum('qhc,khc->hqk', query_heads, key_heads) * 0.125
    key_valid = jnp.arange(key_count, dtype=jnp.int32) < length
    scores = jnp.where(key_valid[None, None, :], scores, -1000000000.0)
    row_max = lax.optimization_barrier(jnp.max(scores, axis=-1, keepdims=True))
    expo = jnp.exp(scores - row_max)
    soft = (expo / lax.optimization_barrier(jnp.sum(expo, axis=-1, keepdims=True))).astype(jnp.bfloat16)
    context = jnp.einsum('hqk,khc->qhc', soft.astype(jnp.float32), value_heads)
    return context.reshape(query_count, head_count * HEAD_DIM).astype(jnp.bfloat16)

def out_terms(context, out_weight):
    row_count = context.shape[0]
    context_groups = context.reshape(row_count, N_FSDP, -1).astype(jnp.float32)
    weight_groups = out_weight.reshape(out_weight.shape[0], N_FSDP, -1).astype(jnp.float32)
    group_terms = jnp.einsum('rgc,dgc->grd', context_groups, weight_groups)
    rounded = lax.optimization_barrier(group_terms.astype(jnp.bfloat16))
    return lax.optimization_barrier(jnp.sum(rounded.astype(jnp.float32), axis=0))

def reference(source_rows, target_rows, attn_weights, gains, lengths):
    half_sections = N_SECTION // 2
    source_blocks = source_rows.reshape(N_SECTION, IN_LEN, D)
    target_blocks = target_rows.reshape(N_SECTION, OUT_LEN, D)
    source_out = []
    target_out = []
    for section_index in range(N_SECTION):
        weights = attn_weights[section_index]
        gain_row = gains[section_index]
        length = lengths[section_index]
        source_block = source_blocks[section_index]
        target_block = target_blocks[section_index]
        if section_index < half_sections:
            normed = rms_norm(source_block, gain_row)
            context = attend(project(normed, weights[0]), project(normed, weights[1]), project(normed, weights[2]), length)
            source_block = (source_block.astype(jnp.float32) + out_terms(context, weights[3])).astype(jnp.bfloat16)
        else:
            normed = rms_norm(target_block, gain_row)
            context = attend(project(normed, weights[0]), project(source_block, weights[1]), project(source_block, weights[2]), length)
            target_block = (target_block.astype(jnp.float32) + out_terms(context, weights[3])).astype(jnp.bfloat16)
        source_out.append(source_block)
        target_out.append(target_block)
    source_next = jnp.roll(jnp.stack(source_out), 1, axis=0).reshape(N_SECTION * IN_LEN, D)
    target_next = jnp.roll(jnp.stack(target_out), 1, axis=0).reshape(N_SECTION * OUT_LEN, D)
    return (source_next, target_next)
```

```python
import functools

import jax
import jax.numpy as jnp
from jax import lax
from jax.experimental import pallas as pl
from jax.experimental.pallas import tpu as pltpu
from jax.sharding import PartitionSpec as P

HEAD_DIM = 64
NX = 4
NZ = 3
NCORE = 2
CHUNKS = 4
MESH = pl.DeviceIdType.MESH


def kernel(
    sections,
    x_hbm,
    y_hbm,
    w_hbm,
    g_hbm,
    len_ref,
    xout,
    yout,
    xin,
    yin,
    gain,
    wqkv,
    wout,
    rows,
    normy,
    accq,
    acckv,
    kv,
    ctx,
    terms,
    r1,
    r2,
    zs,
    part,
    fin,
    ld,
    w_s,
    w_r,
    ag_s,
    az,
    ax,
    af,
    kv_s,
    kv_r,
    e_s,
    e_r,
    rs_s,
    c1,
    c2,
    c3,
    l_s,
    l_r,
    y_s,
    yx,
    yf,
    yp,
):
    own, width = xin.shape
    targets = yin.shape[0]
    lanes = w_hbm.shape[2]
    W = width // CHUNKS
    H = W // 2
    plane = NX * NZ * own
    tplane = NX * own

    s = lax.axis_index("section")
    f = lax.axis_index("fsdp")
    c = lax.rem(f, NCORE)
    zh = lax.rem(f // NCORE, NZ)
    x = f // (NCORE * NZ)
    xr, xl, x2 = lax.rem(x + 1, NX), lax.rem(x + 3, NX), lax.rem(x + 2, NX)
    zu, zd = lax.rem(zh + 1, NZ), lax.rem(zh + 2, NZ)
    s_next, s_prev = lax.rem(s + 1, sections), lax.rem(s + sections - 1, sections)
    enc = s < sections // 2
    dec = jnp.logical_not(enc)
    src_enc = s_prev < sections // 2
    src_dec = jnp.logical_not(src_enc)

    def fid(px, pz, pc):
        return {"fsdp": (px * NZ + pz) * NCORE + pc}

    right, left = fid(xr, zh, c), fid(xl, zh, c)
    up, down = fid(x, zu, c), fid(x, zd, c)
    partner = fid(x, zh, 1 - c)
    forward, backward = {"section": s_next}, {"section": s_prev}
    xdev, xnb = (right, left), (xr, xl)

    def rdma(src, dst, send, recv, dev):
        return pltpu.make_async_remote_copy(
            src_ref=src, dst_ref=dst, send_sem=send, recv_sem=recv, device_id=dev, device_id_type=MESH
        )

    def cols(j):
        return pl.ds(pl.multiple_of(j * W, W), W)

    def half(j, d):
        return pl.ds(pl.multiple_of(j * W + d * H, H), H)

    def blk(k):
        return pl.ds(pl.multiple_of(k * own, own), own)

    ld_x = pltpu.make_async_copy(x_hbm, xin, ld.at[0])
    ld_g = pltpu.make_async_copy(g_hbm, gain, ld.at[1])
    ld_y = pltpu.make_async_copy(y_hbm, yin, ld.at[2])
    ld_x.start()
    ld_g.start()
    ld_y.start()

    barrier = pltpu.get_barrier_semaphore()
    for dev in (partner, right, left, up, down, forward, backward):
        pl.semaphore_signal(barrier, inc=1, device_id=dev, device_id_type=MESH)

    def wslot(i):
        if i < 3:
            return wqkv.at[:, pl.ds(pl.multiple_of(i * NCORE * lanes + c * lanes, lanes), lanes)]
        return wout.at[c]

    ld_w = [pltpu.make_async_copy(w_hbm.at[i], wslot(i), ld.at[3 + i]) for i in range(4)]
    for copy in ld_w:
        copy.start()

    k_own = x * NZ + zh
    ld_x.wait()
    ld_g.wait()

    def normed(block):
        wide = block.astype(jnp.float32)
        inv = lax.rsqrt(jnp.mean(wide * wide, axis=-1, keepdims=True) + 1e-06)
        return (wide * inv * gain[...]).astype(jnp.bfloat16)

    @pl.when(enc)
    def _():
        rows[blk(k_own), :] = normed(xin[...])

    @pl.when(dec)
    def _():
        rows[blk(k_own), :] = xin[...]

    pl.semaphore_wait(barrier, 7)

    zdev = (up, down)
    zb = (zh, zd, zu)
    zfrom = (zd, zu)

    def az_copy(u, j, k):
        ref = rows.at[blk(k), cols(j)]
        return rdma(ref, ref, ag_s, az.at[u, j], zdev[u])

    def ax_copy(b, d, j, k):
        ref = rows.at[blk(k), cols(j)]
        return rdma(ref, ref, ag_s, ax.at[b, d, j], xdev[d])

    def af_copy(b, d, j, k):
        ref = rows.at[blk(k), half(j, d)]
        return rdma(ref, ref, ag_s, af.at[b, d, j], xdev[d])

    @pl.loop(0, CHUNKS)
    def _(j):
        for u in range(2):
            az_copy(u, j, k_own).start()
        for d in range(2):
            ax_copy(0, d, j, k_own).start()

    push_w = [rdma(w_hbm.at[i], wslot(i), w_s, w_r.at[i], partner) for i in range(4)]
    for copy in push_w:
        copy.start()

    ld_y.wait()

    @pl.when(dec)
    def _():
        @pl.loop(0, NX)
        def _(i):
            normy[blk(i), :] = normed(yin[blk(i * NCORE + c), :])

    def relay(b, j):
        for d, origin in ((0, xl), (1, xr)):
            k = origin * NZ + zb[b]
            ax_copy(b, d, j, k).wait_recv()
            af_copy(b, d, j, k).start()

    @pl.loop(0, CHUNKS)
    def _(j):
        relay(0, j)

    accq[...] = jnp.zeros_like(accq)
    acckv[...] = jnp.zeros_like(acckv)
    qw = NCORE * lanes

    @pl.loop(0, CHUNKS + 1)
    def _(j):
        @pl.when(j < CHUNKS)
        def _():
            for u in range(2):
                k = x * NZ + zfrom[u]
                az_copy(u, j, k).wait_recv()
                for d in range(2):
                    ax_copy(1 + u, d, j, k).start()
            for b in (1, 2):
                relay(b, j)

        @pl.when(j == 0)
        def _():
            for i in range(3):
                ld_w[i].wait()
                push_w[i].wait_recv()

        @pl.when(j > 0)
        def _():
            jj = j - 1
            for b in range(3):
                for d in range(2):
                    af_copy(b, d, jj, x2 * NZ + zb[b]).wait_recv()
            wc = wqkv.at[cols(jj), :]
            acckv[...] += jnp.dot(rows[:, cols(jj)], wc[:, qw:], preferred_element_type=jnp.float32)

            @pl.when(enc)
            def _():
                accq[...] += jnp.dot(rows[:, cols(jj)], wc[:, :qw], preferred_element_type=jnp.float32)

            @pl.when(dec)
            def _():
                accq[:tplane, :] += jnp.dot(
                    normy[:, cols(jj)], wc[:, :qw], preferred_element_type=jnp.float32
                )

    m_own = x * NCORE + c
    early_enc = rdma(yin.at[blk(m_own)], yout.at[blk(m_own)], e_s, e_r, forward)
    early_dec = rdma(xin, xout, e_s, e_r, forward)

    @pl.when(enc)
    def _():
        early_enc.start()

    @pl.when(dec)
    def _():
        early_dec.start()

    kv_rows = pl.ds(pl.multiple_of(c * plane, plane), plane)
    kv[kv_rows, :] = acckv[...].astype(jnp.bfloat16)
    kv_copy = rdma(kv.at[kv_rows], kv.at[kv_rows], kv_s, kv_r, partner)
    kv_copy.start()
    kv_copy.wait_recv()

    keys = NCORE * plane
    length = len_ref[0]
    n = lax.broadcasted_iota(jnp.int32, (1, keys), 1)
    p_of = (n >= plane).astype(jnp.int32)
    r_of = n - p_of * plane
    position = (r_of // own) * (NCORE * own) + p_of * own + (r_of & (own - 1))
    valid = position < length

    def attention(mq):
        lane = lax.broadcasted_iota(jnp.int32, (mq, lanes), 1)
        for p in range(NCORE):
            qp = accq[:mq, p * lanes : (p + 1) * lanes].astype(jnp.bfloat16)
            kp = kv[:, p * lanes : (p + 1) * lanes]
            vp = kv[:, qw + p * lanes : qw + (p + 1) * lanes]
            outs = []
            for h in range(lanes // HEAD_DIM):
                mine = (lane >= h * HEAD_DIM) & (lane < (h + 1) * HEAD_DIM)
                qh = jnp.where(mine, qp, jnp.zeros_like(qp))
                sc = lax.dot_general(
                    qh, kp, (((1,), (1,)), ((), ())), preferred_element_type=jnp.float32
                )
                sc = jnp.where(valid, sc * 0.125, -1000000000.0)
                ex = jnp.exp(sc - jnp.max(sc, axis=-1, keepdims=True))
                soft = (ex / jnp.sum(ex, axis=-1, keepdims=True)).astype(jnp.bfloat16)
                outs.append(jnp.dot(soft, vp, preferred_element_type=jnp.float32))
            both = outs[0]
            for h in range(1, len(outs)):
                both = jnp.where(lane >= h * HEAD_DIM, outs[h], both)
            ctx[:mq, p * lanes : (p + 1) * lanes] = both.astype(jnp.bfloat16)

    zr = (zu, zd, zh)

    def project(mq, j):
        total = None
        for p in range(NCORE):
            term = lax.dot_general(
                ctx[:mq, p * lanes : (p + 1) * lanes],
                wout[p, cols(j), :],
                (((1,), (1,)), ((), ())),
                preferred_element_type=jnp.float32,
            )
            term = term.astype(jnp.bfloat16).astype(jnp.float32)
            total = term if total is None else total + term
        terms[:mq, cols(j)] = total.astype(jnp.bfloat16)

    def reduction(tblk):
        def c1_copy(r, d, j):
            return rdma(
                terms.at[tblk(x2, r), half(j, d)], r1.at[r, :, half(j, d)], rs_s, c1.at[r, d, j], xdev[d]
            )

        def c2_copy(r, d, j):
            return rdma(
                terms.at[tblk(xnb[d], r), cols(j)], r2.at[r, d, :, cols(j)], rs_s, c2.at[r, d, j], xdev[d]
            )

        def first(r, j):
            for d in range(2):
                c1_copy(r, d, j).start()

        def second(r, j):
            for d in range(2):
                c1_copy(r, d, j).wait_recv()
                at = (tblk(xnb[d], r), half(j, d))
                terms[at] = (
                    terms[at].astype(jnp.float32) + r1[r, :, half(j, d)].astype(jnp.float32)
                ).astype(jnp.bfloat16)
                c2_copy(r, d, j).start()

        def third(r, j):
            for d in range(2):
                c2_copy(r, d, j).wait_recv()
            return (
                terms[tblk(x, r), cols(j)].astype(jnp.float32)
                + r2[r, 0, :, cols(j)].astype(jnp.float32)
                + r2[r, 1, :, cols(j)].astype(jnp.float32)
            ).astype(jnp.bfloat16)

        return first, second, third

    def z_copy(src, u, j, slot):
        return rdma(src, part.at[slot, :, cols(j)], rs_s, c3.at[u, j], zdev[u])

    @pl.when(enc)
    def _():
        attention(plane)
        ld_w[3].wait()
        push_w[3].wait_recv()
        first, second, third = reduction(lambda px, r: blk(px * NZ + zr[r]))

        @pl.loop(0, CHUNKS + 2)
        def _(j):
            @pl.when(j < CHUNKS)
            def _():
                project(plane, j)
                for r in range(2):
                    first(r, j)

            @pl.when((j >= 1) & (j < CHUNKS + 1))
            def _():
                for r in range(2):
                    second(r, j - 1)

            @pl.when(j >= 2)
            def _():
                for u in range(2):
                    zs[u, :, cols(j - 2)] = third(u, j - 2)
                    z_copy(zs.at[u, :, cols(j - 2)], u, j - 2, zh).start()

        @pl.loop(0, CHUNKS)
        def _(j):
            first(2, j)

        @pl.loop(0, CHUNKS)
        def _(j):
            second(2, j)

        @pl.loop(0, CHUNKS)
        def _(j):
            part[zh, :, cols(j)] = third(2, j)

    @pl.when(dec)
    def _():
        attention(tplane)
        ld_w[3].wait()
        push_w[3].wait_recv()
        first, second, third = reduction(lambda px, r: blk(px))

        @pl.loop(0, CHUNKS + 2)
        def _(j):
            @pl.when(j < CHUNKS)
            def _():
                project(tplane, j)
                first(2, j)

            @pl.when((j >= 1) & (j < CHUNKS + 1))
            def _():
                second(2, j - 1)

            @pl.when(j >= 2)
            def _():
                part[zh, :, cols(j - 2)] = third(2, j - 2)
                for u in range(2):
                    z_copy(part.at[zh, :, cols(j - 2)], u, j - 2, zh).start()

    def yx_copy(d, j, m):
        ref = yout.at[blk(m), cols(j)]
        return rdma(ref, ref, y_s, yx.at[d, j], xdev[d])

    def yf_copy(d, j, m):
        ref = yout.at[blk(m), half(j, d)]
        return rdma(ref, ref, y_s, yf.at[d, j], xdev[d])

    def yp_copy(i, j, m):
        ref = yout.at[blk(m), cols(j)]
        return rdma(ref, ref, y_s, yp.at[i, j], partner)

    def late_recv(j):
        rdma(fin.at[:, cols(j)], fin.at[:, cols(j)], l_s, l_r.at[j], forward).wait_recv()

    def spread(arrived):
        @pl.loop(0, CHUNKS)
        def _(j):
            arrived(j)
            for d in range(2):
                yx_copy(d, j, m_own).start()
            yp_copy(0, j, m_own).start()

        @pl.loop(0, CHUNKS)
        def _(j):
            for d, origin in ((0, xl), (1, xr)):
                m = origin * NCORE + c
                yx_copy(d, j, m).wait_recv()
                yf_copy(d, j, m).start()
                yp_copy(1 + d, j, m).start()

        @pl.loop(0, CHUNKS)
        def _(j):
            m = x2 * NCORE + c
            for d in range(2):
                yf_copy(d, j, m).wait_recv()
            yp_copy(3, j, m).start()

    @pl.when(src_enc)
    def _():
        early_dec.wait_recv()
        spread(lambda j: None)

    def late_copy(j, dst):
        return rdma(fin.at[:, cols(j)], dst, l_s, l_r.at[j], forward)

    @pl.loop(0, CHUNKS)
    def _(j):
        for u in range(2):
            z_copy(part.at[zfrom[u], :, cols(j)], u, j, zfrom[u]).wait_recv()
        delta = (
            part[0, :, cols(j)].astype(jnp.float32)
            + part[1, :, cols(j)].astype(jnp.float32)
            + part[2, :, cols(j)].astype(jnp.float32)
        )

        @pl.when(enc)
        def _():
            fin[:, cols(j)] = (xin[:, cols(j)].astype(jnp.float32) + delta).astype(jnp.bfloat16)
            late_copy(j, xout.at[:, cols(j)]).start()

        @pl.when(dec)
        def _():
            fin[:, cols(j)] = (yin[blk(m_own), cols(j)].astype(jnp.float32) + delta).astype(
                jnp.bfloat16
            )
            late_copy(j, yout.at[blk(m_own), cols(j)]).start()

    @pl.when(src_dec)
    def _():
        spread(late_recv)
        early_dec.wait_recv()

    @pl.when(src_enc)
    def _():
        @pl.loop(0, CHUNKS)
        def _(j):
            late_recv(j)

    @pl.loop(0, CHUNKS)
    def _(j):
        for i, px in enumerate((x, xl, xr, x2)):
            yp_copy(i, j, px * NCORE + 1 - c).wait_recv()

    def drain(ref, sem):
        pltpu.make_async_copy(ref, ref, sem).wait()

    drain(wqkv.at[:, : 4 * lanes], w_s)
    drain(rows.at[: 11 * own], ag_s)
    drain(kv.at[:plane], kv_s)
    drain(xin, e_s)
    drain(fin, l_s)
    drain(yout.at[: 7 * own], y_s)

    @pl.when(enc)
    def _():
        drain(terms.at[: 11 * own], rs_s)

    @pl.when(dec)
    def _():
        drain(terms.at[: 5 * own], rs_s)


def local(sections, source_rows, target_rows, attn_weights, gains, lengths):
    weights = attn_weights[0]
    own, width = source_rows.shape
    targets = target_rows.shape[0]
    lanes = weights.shape[2]
    plane = NX * NZ * own
    tplane = NX * own
    bf, f32 = jnp.bfloat16, jnp.float32
    vmem = pltpu.VMEM
    dma = pltpu.SemaphoreType.DMA
    return pl.pallas_call(
        functools.partial(kernel, sections),
        out_shape=(
            jax.ShapeDtypeStruct((own, width), bf),
            jax.ShapeDtypeStruct((targets, width), bf),
        ),
        in_specs=[pl.BlockSpec(memory_space=pl.ANY)] * 4 + [pl.BlockSpec(memory_space=pltpu.SMEM)],
        out_specs=(pl.BlockSpec(memory_space=vmem), pl.BlockSpec(memory_space=vmem)),
        scratch_shapes=[
            vmem((own, width), bf),
            vmem((targets, width), bf),
            vmem((1, width), f32),
            vmem((width, 3 * NCORE * lanes), bf),
            vmem((NCORE, width, lanes), bf),
            vmem((plane, width), bf),
            vmem((tplane, width), bf),
            vmem((plane, NCORE * lanes), f32),
            vmem((plane, 2 * NCORE * lanes), f32),
            vmem((NCORE * plane, 2 * NCORE * lanes), bf),
            vmem((plane, NCORE * lanes), bf),
            vmem((plane, width), bf),
            vmem((3, own, width), bf),
            vmem((3, 2, own, width), bf),
            vmem((2, own, width), bf),
            vmem((NZ, own, width), bf),
            vmem((own, width), bf),
            dma((7,)),
            dma(()),
            dma((4,)),
            dma(()),
            dma((2, CHUNKS)),
            dma((3, 2, CHUNKS)),
            dma((3, 2, CHUNKS)),
            dma(()),
            dma(()),
            dma(()),
            dma(()),
            dma(()),
            dma((3, 2, CHUNKS)),
            dma((3, 2, CHUNKS)),
            dma((2, CHUNKS)),
            dma(()),
            dma((CHUNKS,)),
            dma(()),
            dma((2, CHUNKS)),
            dma((2, CHUNKS)),
            dma((4, CHUNKS)),
        ],
        compiler_params=pltpu.CompilerParams(
            collective_id=0, has_side_effects=True, vmem_limit_bytes=56 * 1024 * 1024
        ),
        name="tick",
    )(source_rows, target_rows, weights, gains, lengths)


def solution(mesh):
    in_specs = (
        P(("section", "fsdp"), None),
        P("section", None),
        P("section", None, None, "fsdp"),
        P("section", None),
        P("section"),
    )
    out_specs = (P(("section", "fsdp"), None), P("section", None))
    body = functools.partial(local, mesh.shape["section"])
    return jax.shard_map(body, mesh=mesh, in_specs=in_specs, out_specs=out_specs, check_vma=False)
```

```python
import contextlib
import functools

import jax
import jax.numpy as jnp
from jax import lax
from jax.experimental import pallas as pl
from jax.experimental.pallas import tpu as pltpu
from jax.sharding import PartitionSpec as P

HEAD_DIM = 64
NX = 4
NZ = 3
NCORE = 2
CHUNKS = 4
GATHER_LAG = 4
REDUCE_LAG = 4
SPREAD_LAG = 4
MESH = pl.DeviceIdType.MESH


def scope(name):
    return contextlib.nullcontext()


def kernel(
    sections,
    x_hbm,
    y_hbm,
    w_hbm,
    g_hbm,
    len_hbm,
    xout,
    yout,
    xin,
    yin,
    gain,
    len_ref,
    wqkv,
    wout,
    rows,
    normy,
    accq,
    acckv,
    kv,
    ctx,
    terms,
    r1,
    r2,
    zs,
    part,
    fin,
    ld,
    w_s,
    w_r,
    ag_s,
    az,
    ax,
    af,
    kv_s,
    kv_r,
    e_s,
    e_r,
    rs_s,
    c1,
    c2,
    c3,
    l_s,
    l_r,
    y_s,
    yx,
    yf,
    yp,
):
    own, width = xin.shape
    targets = yin.shape[0]
    lanes = w_hbm.shape[2]
    W = width // CHUNKS
    H = W // 2
    plane = NX * NZ * own
    tplane = NX * own

    s = lax.axis_index("section")
    f = lax.axis_index("fsdp")
    c = lax.rem(f, NCORE)
    zh = lax.rem(f // NCORE, NZ)
    x = f // (NCORE * NZ)
    xr, xl, x2 = lax.rem(x + 1, NX), lax.rem(x + 3, NX), lax.rem(x + 2, NX)
    zu, zd = lax.rem(zh + 1, NZ), lax.rem(zh + 2, NZ)
    s_next, s_prev = lax.rem(s + 1, sections), lax.rem(s + sections - 1, sections)
    enc = s < sections // 2
    dec = jnp.logical_not(enc)
    src_enc = s_prev < sections // 2
    src_dec = jnp.logical_not(src_enc)

    def fid(px, pz, pc):
        return {"fsdp": (px * NZ + pz) * NCORE + pc}

    right, left = fid(xr, zh, c), fid(xl, zh, c)
    up, down = fid(x, zu, c), fid(x, zd, c)
    partner = fid(x, zh, 1 - c)
    forward, backward = {"section": s_next}, {"section": s_prev}
    xdev, xnb = (right, left), (xr, xl)

    def rdma(src, dst, send, recv, dev):
        return pltpu.make_async_remote_copy(
            src_ref=src, dst_ref=dst, send_sem=send, recv_sem=recv, device_id=dev, device_id_type=MESH
        )

    def cols(j):
        return pl.ds(pl.multiple_of(j * W, W), W)

    def half(j, d):
        return pl.ds(pl.multiple_of(j * W + d * H, H), H)

    def blk(k):
        return pl.ds(pl.multiple_of(k * own, own), own)

    ld_x = pltpu.make_async_copy(x_hbm, xin, ld.at[0])
    ld_g = pltpu.make_async_copy(g_hbm, gain, ld.at[1])
    ld_y = pltpu.make_async_copy(y_hbm, yin, ld.at[2])
    ld_x.start()
    ld_g.start()
    ld_y.start()
    ld_n = pltpu.make_async_copy(len_hbm, len_ref, ld.at[7])
    ld_n.start()

    barrier = pltpu.get_barrier_semaphore()
    for dev in (partner, right, left, up, down, forward, backward):
        pl.semaphore_signal(barrier, inc=1, device_id=dev, device_id_type=MESH)

    def wslot(i):
        if i < 3:
            return wqkv.at[:, pl.ds(pl.multiple_of(i * NCORE * lanes + c * lanes, lanes), lanes)]
        return wout.at[c]

    ld_w = [pltpu.make_async_copy(w_hbm.at[i], wslot(i), ld.at[3 + i]) for i in range(4)]
    for copy in ld_w:
        copy.start()

    k_own = x * NZ + zh
    with scope("ld"):
        ld_x.wait()
        ld_g.wait()

    def normed(block):
        wide = block.astype(jnp.float32)
        inv = lax.rsqrt(jnp.mean(wide * wide, axis=-1, keepdims=True) + 1e-06)
        return (wide * inv * gain[...]).astype(jnp.bfloat16)

    @pl.when(enc)
    def _():
        rows[blk(k_own), :] = normed(xin[...])

    @pl.when(dec)
    def _():
        rows[blk(k_own), :] = xin[...]

    with scope("barrier"):
        pl.semaphore_wait(barrier, 7)

    zdev = (up, down)
    zb = (zh, zd, zu)
    zfrom = (zd, zu)

    def az_copy(u, j, k):
        ref = rows.at[blk(k), cols(j)]
        return rdma(ref, ref, ag_s, az.at[u, j], zdev[u])

    def ax_copy(b, d, j, k):
        ref = rows.at[blk(k), cols(j)]
        return rdma(ref, ref, ag_s, ax.at[b, d, j], xdev[d])

    def af_copy(b, d, j, k):
        ref = rows.at[blk(k), half(j, d)]
        return rdma(ref, ref, ag_s, af.at[b, d, j], xdev[d])

    @pl.loop(0, CHUNKS)
    def _(j):
        for u in range(2):
            az_copy(u, j, k_own).start()
        for d in range(2):
            ax_copy(0, d, j, k_own).start()

    push_w = [rdma(w_hbm.at[i], wslot(i), w_s, w_r.at[i], partner) for i in range(4)]
    for copy in push_w:
        copy.start()

    ld_y.wait()

    @pl.when(dec)
    def _():
        with scope("normy"):

            @pl.loop(0, NX)
            def _(i):
                normy[blk(i), :] = normed(yin[blk(i * NCORE + c), :])

    def relay(b, j):
        for d, origin in ((0, xl), (1, xr)):
            k = origin * NZ + zb[b]
            ax_copy(b, d, j, k).wait_recv()
            af_copy(b, d, j, k).start()

    @pl.loop(0, CHUNKS)
    def _(j):
        with scope("relay0"):
            relay(0, j)

    accq[...] = jnp.zeros_like(accq)
    acckv[...] = jnp.zeros_like(acckv)
    qw = NCORE * lanes

    @pl.loop(0, CHUNKS + 2 * GATHER_LAG)
    def _(j):
        @pl.when(j < CHUNKS)
        def _():
            for u in range(2):
                k = x * NZ + zfrom[u]
                with scope("az_wait"):
                    az_copy(u, j, k).wait_recv()
                for d in range(2):
                    ax_copy(1 + u, d, j, k).start()

        @pl.when((j >= GATHER_LAG) & (j < CHUNKS + GATHER_LAG))
        def _():
            with scope("relay12"):
                for b in (1, 2):
                    relay(b, j - GATHER_LAG)

        @pl.when(j == 0)
        def _():
            with scope("w_wait"):
                for i in range(3):
                    ld_w[i].wait()
                    push_w[i].wait_recv()

        @pl.when(j >= 2 * GATHER_LAG)
        def _():
            jj = j - 2 * GATHER_LAG
            with scope("af_wait"):
                for b in range(3):
                    for d in range(2):
                        af_copy(b, d, jj, x2 * NZ + zb[b]).wait_recv()
            wc = wqkv.at[cols(jj), :]
            acckv[...] += jnp.dot(rows[:, cols(jj)], wc[:, qw:], preferred_element_type=jnp.float32)

            @pl.when(enc)
            def _():
                accq[...] += jnp.dot(rows[:, cols(jj)], wc[:, :qw], preferred_element_type=jnp.float32)

            @pl.when(dec)
            def _():
                accq[:tplane, :] += jnp.dot(
                    normy[:, cols(jj)], wc[:, :qw], preferred_element_type=jnp.float32
                )

    m_own = x * NCORE + c
    early_enc = rdma(yin.at[blk(m_own)], yout.at[blk(m_own)], e_s, e_r, forward)
    early_dec = rdma(xin, xout, e_s, e_r, forward)

    @pl.when(enc)
    def _():
        early_enc.start()

    @pl.when(dec)
    def _():
        early_dec.start()

    kv_rows = pl.ds(pl.multiple_of(c * plane, plane), plane)
    kv[kv_rows, :] = acckv[...].astype(jnp.bfloat16)
    kv_copy = rdma(kv.at[kv_rows], kv.at[kv_rows], kv_s, kv_r, partner)
    kv_copy.start()
    with scope("kv_wait"):
        kv_copy.wait_recv()

    keys = NCORE * plane
    ld_n.wait()
    length = len_ref[0]
    n = lax.broadcasted_iota(jnp.int32, (1, keys), 1)
    p_of = (n >= plane).astype(jnp.int32)
    r_of = n - p_of * plane
    position = (r_of // own) * (NCORE * own) + p_of * own + (r_of & (own - 1))
    valid = position < length

    def attention(mq):
        lane = lax.broadcasted_iota(jnp.int32, (mq, lanes), 1)
        for p in range(NCORE):
            qp = accq[:mq, p * lanes : (p + 1) * lanes].astype(jnp.bfloat16)
            kp = kv[:, p * lanes : (p + 1) * lanes]
            vp = kv[:, qw + p * lanes : qw + (p + 1) * lanes]
            outs = []
            for h in range(lanes // HEAD_DIM):
                mine = (lane >= h * HEAD_DIM) & (lane < (h + 1) * HEAD_DIM)
                qh = jnp.where(mine, qp, jnp.zeros_like(qp))
                sc = lax.dot_general(
                    qh, kp, (((1,), (1,)), ((), ())), preferred_element_type=jnp.float32
                )
                sc = jnp.where(valid, sc * 0.125, -1000000000.0)
                ex = jnp.exp(sc - jnp.max(sc, axis=-1, keepdims=True))
                soft = (ex / jnp.sum(ex, axis=-1, keepdims=True)).astype(jnp.bfloat16)
                outs.append(jnp.dot(soft, vp, preferred_element_type=jnp.float32))
            both = outs[0]
            for h in range(1, len(outs)):
                both = jnp.where(lane >= h * HEAD_DIM, outs[h], both)
            ctx[:mq, p * lanes : (p + 1) * lanes] = both.astype(jnp.bfloat16)

    zr = (zu, zd, zh)

    def project(mq, j):
        total = None
        for p in range(NCORE):
            term = lax.dot_general(
                ctx[:mq, p * lanes : (p + 1) * lanes],
                wout[p, cols(j), :],
                (((1,), (1,)), ((), ())),
                preferred_element_type=jnp.float32,
            )
            term = term.astype(jnp.bfloat16).astype(jnp.float32)
            total = term if total is None else total + term
        terms[:mq, cols(j)] = total.astype(jnp.bfloat16)

    def reduction(tblk):
        def c1_copy(r, d, j):
            return rdma(
                terms.at[tblk(x2, r), half(j, d)], r1.at[r, :, half(j, d)], rs_s, c1.at[r, d, j], xdev[d]
            )

        def c2_copy(r, d, j):
            return rdma(
                terms.at[tblk(xnb[d], r), cols(j)], r2.at[r, d, :, cols(j)], rs_s, c2.at[r, d, j], xdev[d]
            )

        def first(r, j):
            for d in range(2):
                c1_copy(r, d, j).start()

        def second(r, j):
            for d in range(2):
                c1_copy(r, d, j).wait_recv()
                at = (tblk(xnb[d], r), half(j, d))
                terms[at] = (
                    terms[at].astype(jnp.float32) + r1[r, :, half(j, d)].astype(jnp.float32)
                ).astype(jnp.bfloat16)
                c2_copy(r, d, j).start()

        def third(r, j):
            for d in range(2):
                c2_copy(r, d, j).wait_recv()
            return (
                terms[tblk(x, r), cols(j)].astype(jnp.float32)
                + r2[r, 0, :, cols(j)].astype(jnp.float32)
                + r2[r, 1, :, cols(j)].astype(jnp.float32)
            ).astype(jnp.bfloat16)

        return first, second, third

    def z_copy(src, u, j, slot):
        return rdma(src, part.at[slot, :, cols(j)], rs_s, c3.at[u, j], zdev[u])

    @pl.when(enc)
    def _():
        with scope("attention"):
            attention(plane)
        ld_w[3].wait()
        push_w[3].wait_recv()
        first, second, third = reduction(lambda px, r: blk(px * NZ + zr[r]))

        @pl.loop(0, 2 * CHUNKS + 2 * REDUCE_LAG)
        def _(i):
            @pl.when(i < CHUNKS)
            def _():
                with scope("project"):
                    project(plane, i)
                for r in range(2):
                    first(r, i)

            @pl.when((i >= CHUNKS) & (i < 2 * CHUNKS))
            def _():
                first(2, i - CHUNKS)

            @pl.when((i >= REDUCE_LAG) & (i < CHUNKS + REDUCE_LAG))
            def _():
                with scope("second"):
                    for r in range(2):
                        second(r, i - REDUCE_LAG)

            @pl.when((i >= CHUNKS + REDUCE_LAG) & (i < 2 * CHUNKS + REDUCE_LAG))
            def _():
                with scope("second_own"):
                    second(2, i - CHUNKS - REDUCE_LAG)

            @pl.when((i >= 2 * REDUCE_LAG) & (i < CHUNKS + 2 * REDUCE_LAG))
            def _():
                j = i - 2 * REDUCE_LAG
                for u in range(2):
                    with scope("third"):
                        zs[u, :, cols(j)] = third(u, j)
                    z_copy(zs.at[u, :, cols(j)], u, j, zh).start()

            @pl.when(i >= CHUNKS + 2 * REDUCE_LAG)
            def _():
                j = i - CHUNKS - 2 * REDUCE_LAG
                with scope("third_own"):
                    part[zh, :, cols(j)] = third(2, j)

    @pl.when(dec)
    def _():
        with scope("attention"):
            attention(tplane)
        ld_w[3].wait()
        push_w[3].wait_recv()
        first, second, third = reduction(lambda px, r: blk(px))

        @pl.loop(0, CHUNKS + 2 * REDUCE_LAG)
        def _(i):
            @pl.when(i < CHUNKS)
            def _():
                with scope("project"):
                    project(tplane, i)
                first(2, i)

            @pl.when((i >= REDUCE_LAG) & (i < CHUNKS + REDUCE_LAG))
            def _():
                with scope("second"):
                    second(2, i - REDUCE_LAG)

            @pl.when(i >= 2 * REDUCE_LAG)
            def _():
                j = i - 2 * REDUCE_LAG
                with scope("third"):
                    part[zh, :, cols(j)] = third(2, j)
                for u in range(2):
                    z_copy(part.at[zh, :, cols(j)], u, j, zh).start()

    def yx_copy(d, j, m):
        ref = yout.at[blk(m), cols(j)]
        return rdma(ref, ref, y_s, yx.at[d, j], xdev[d])

    def yf_copy(d, j, m):
        ref = yout.at[blk(m), half(j, d)]
        return rdma(ref, ref, y_s, yf.at[d, j], xdev[d])

    def yp_copy(i, j, m):
        ref = yout.at[blk(m), cols(j)]
        return rdma(ref, ref, y_s, yp.at[i, j], partner)

    def late_recv(j):
        rdma(fin.at[:, cols(j)], fin.at[:, cols(j)], l_s, l_r.at[j], forward).wait_recv()

    def spread_first(j):
        for d in range(2):
            yx_copy(d, j, m_own).start()
        yp_copy(0, j, m_own).start()

    def spread_second(j):
        for d, origin in ((0, xl), (1, xr)):
            m = origin * NCORE + c
            with scope("yx_wait"):
                yx_copy(d, j, m).wait_recv()
            yf_copy(d, j, m).start()
            yp_copy(1 + d, j, m).start()

    def spread_third(j):
        m = x2 * NCORE + c
        with scope("yf_wait"):
            for d in range(2):
                yf_copy(d, j, m).wait_recv()
        yp_copy(3, j, m).start()

    @pl.when(src_enc)
    def _():
        with scope("early_wait"):
            early_dec.wait_recv()

        @pl.loop(0, CHUNKS)
        def _(j):
            spread_first(j)

    def late_copy(j, dst):
        return rdma(fin.at[:, cols(j)], dst, l_s, l_r.at[j], forward)

    @pl.loop(0, CHUNKS)
    def _(j):
        with scope("z_wait"):
            for u in range(2):
                z_copy(part.at[zfrom[u], :, cols(j)], u, j, zfrom[u]).wait_recv()
        delta = (
            part[0, :, cols(j)].astype(jnp.float32)
            + part[1, :, cols(j)].astype(jnp.float32)
            + part[2, :, cols(j)].astype(jnp.float32)
        )

        @pl.when(enc)
        def _():
            fin[:, cols(j)] = (xin[:, cols(j)].astype(jnp.float32) + delta).astype(jnp.bfloat16)
            late_copy(j, xout.at[:, cols(j)]).start()

        @pl.when(dec)
        def _():
            fin[:, cols(j)] = (yin[blk(m_own), cols(j)].astype(jnp.float32) + delta).astype(
                jnp.bfloat16
            )
            late_copy(j, yout.at[blk(m_own), cols(j)]).start()

    @pl.when(src_dec)
    def _():
        @pl.loop(0, CHUNKS + 2 * SPREAD_LAG)
        def _(j):
            @pl.when(j < CHUNKS)
            def _():
                with scope("late_wait"):
                    late_recv(j)
                spread_first(j)

            @pl.when((j >= SPREAD_LAG) & (j < CHUNKS + SPREAD_LAG))
            def _():
                spread_second(j - SPREAD_LAG)

            @pl.when(j >= 2 * SPREAD_LAG)
            def _():
                spread_third(j - 2 * SPREAD_LAG)

        early_dec.wait_recv()

    @pl.when(src_enc)
    def _():
        @pl.loop(0, CHUNKS)
        def _(j):
            spread_second(j)

        @pl.loop(0, CHUNKS)
        def _(j):
            spread_third(j)

        @pl.loop(0, CHUNKS)
        def _(j):
            with scope("late_wait"):
                late_recv(j)

    @pl.loop(0, CHUNKS)
    def _(j):
        with scope("yp_wait"):
            for i, px in enumerate((x, xl, xr, x2)):
                yp_copy(i, j, px * NCORE + 1 - c).wait_recv()

    def drain(ref, sem):
        pltpu.make_async_copy(ref, ref, sem).wait()

    with scope("drain0"):
        drain(wqkv.at[:, : 4 * lanes], w_s)
    drain(rows.at[: 11 * own], ag_s)
    drain(kv.at[:plane], kv_s)
    drain(xin, e_s)
    drain(fin, l_s)
    drain(yout.at[: 7 * own], y_s)

    @pl.when(enc)
    def _():
        drain(terms.at[: 11 * own], rs_s)

    @pl.when(dec)
    def _():
        drain(terms.at[: 5 * own], rs_s)


def write_out(x_ref, y_ref, x_out, y_out, sem):
    copies = [
        pltpu.make_async_copy(x_ref, x_out, sem.at[0]),
        pltpu.make_async_copy(y_ref, y_out, sem.at[1]),
    ]
    for copy in copies:
        copy.start()
    for copy in copies:
        copy.wait()


def local(sections, source_rows, target_rows, attn_weights, gains, lengths):
    weights = attn_weights[0]
    own, width = source_rows.shape
    targets = target_rows.shape[0]
    lanes = weights.shape[2]
    plane = NX * NZ * own
    tplane = NX * own
    bf, f32 = jnp.bfloat16, jnp.float32
    vmem = pltpu.VMEM
    dma = pltpu.SemaphoreType.DMA
    results = pl.pallas_call(
        functools.partial(kernel, sections),
        out_shape=(vmem((own, width), bf), vmem((targets, width), bf)),
        in_specs=[pl.BlockSpec(memory_space=pltpu.HBM)] * 5,
        out_specs=(pl.BlockSpec(memory_space=vmem), pl.BlockSpec(memory_space=vmem)),
        scratch_shapes=[
            vmem((own, width), bf),
            vmem((targets, width), bf),
            vmem((1, width), f32),
            pltpu.SMEM((1,), jnp.int32),
            vmem((width, 3 * NCORE * lanes), bf),
            vmem((NCORE, width, lanes), bf),
            vmem((plane, width), bf),
            vmem((tplane, width), bf),
            vmem((plane, NCORE * lanes), f32),
            vmem((plane, 2 * NCORE * lanes), f32),
            vmem((NCORE * plane, 2 * NCORE * lanes), bf),
            vmem((plane, NCORE * lanes), bf),
            vmem((plane, width), bf),
            vmem((3, own, width), bf),
            vmem((3, 2, own, width), bf),
            vmem((2, own, width), bf),
            vmem((NZ, own, width), bf),
            vmem((own, width), bf),
            dma((8,)),
            dma(()),
            dma((4,)),
            dma(()),
            dma((2, CHUNKS)),
            dma((3, 2, CHUNKS)),
            dma((3, 2, CHUNKS)),
            dma(()),
            dma(()),
            dma(()),
            dma(()),
            dma(()),
            dma((3, 2, CHUNKS)),
            dma((3, 2, CHUNKS)),
            dma((2, CHUNKS)),
            dma(()),
            dma((CHUNKS,)),
            dma(()),
            dma((2, CHUNKS)),
            dma((2, CHUNKS)),
            dma((4, CHUNKS)),
        ],
        compiler_params=pltpu.CompilerParams(
            collective_id=0, has_side_effects=True, vmem_limit_bytes=56 * 1024 * 1024
        ),
        name="tick",
    )(source_rows, target_rows, weights, gains, lengths)
    return pl.pallas_call(
        write_out,
        out_shape=(
            jax.ShapeDtypeStruct((own, width), bf),
            jax.ShapeDtypeStruct((targets, width), bf),
        ),
        in_specs=[pl.BlockSpec(memory_space=vmem)] * 2,
        out_specs=(pl.BlockSpec(memory_space=pl.ANY), pl.BlockSpec(memory_space=pl.ANY)),
        scratch_shapes=[dma((2,))],
        compiler_params=pltpu.CompilerParams(vmem_limit_bytes=1024 * 1024),
        name="write_out",
    )(*results)


def solution(mesh):
    in_specs = (
        P(("section", "fsdp"), None),
        P("section", None),
        P("section", None, None, "fsdp"),
        P("section", None),
        P("section"),
    )
    out_specs = (P(("section", "fsdp"), None), P("section", None))
    body = functools.partial(local, mesh.shape["section"])
    return jax.shard_map(body, mesh=mesh, in_specs=in_specs, out_specs=out_specs, check_vma=False)
```
